32 devices in a mesh: section: 2 (over x), dp: 16 (over z, y, core).
Axes of the slice: x: 2, y: 2, z: 4, core: 2. Of those that a mesh axis runs over, the one named last changes fastest.
Arguments:
- ln_input: bfloat16 [2, 2048, 12288], P('section', 'dp'), may hold values from -6 to 6
- ln_grad: bfloat16 [2, 2048, 12288], P('section', 'dp'), may hold values from -6 to 6
- top_grad: bfloat16 [2, 2048, 12288], P('section', 'dp'), may hold values from -6 to 6
- ln_gain: float32 [2, 12288], P('section'), may hold values from 0.1 to 1.9
- hidden: bfloat16 [2, 2048, 32], P('section', 'dp'), may hold values from -8 to 8
- master: float32 [2, 32, 12288], P('section', 'dp'), may hold values from -6 to 6
- moment: float32 [2, 32, 12288], P('section', 'dp'), may hold values from -6 to 6
- second: float32 [2, 32, 12288], P('section', 'dp'), may hold values from 0.1 to 4
Outputs:
- new_master: float32 [2, 32, 12288], P('section', 'dp')
- new_moment: float32 [2, 32, 12288], P('section', 'dp')
- new_second: float32 [2, 32, 12288], P('section', 'dp')
- weights: bfloat16 [2, 32, 12288], P('section')
The draws below stay inside these ranges and needn't reach their ends.
All inputs are finite; a program needn't handle non-finite values.
Results may differ from the reference program's by a relative error of at most 0.0078.
Values may be sent and summed in bfloat16 or wider, within the bound.
A program may use at most 64 MiB of HBM per device.

```python
import math
import jax
import jax.numpy as jnp
from jax import lax

D = 12288
STEP = 20
TOKENS = 2048
ROWS = 32
N_SECTION = 2


def draw_hidden(key, part):
    keys = jax.random.split(key, 4)
    base = jax.random.normal(keys[0], (N_SECTION, TOKENS, ROWS), jnp.float32)
    position = jnp.arange(ROWS, dtype=jnp.float32) / max(ROWS - 1, 1)
    level = jnp.arange(N_SECTION, dtype=jnp.float32) / max(N_SECTION - 1, 1)
    column = 3.0 ** position * jax.random.uniform(keys[3], (ROWS,), jnp.float32, 0.5, 1.5)
    scaled = base * column[None, None, :] * (3.0 ** level)[:, None, None] / math.sqrt(TOKENS)
    return jnp.clip(scaled, -8.0, 8.0).astype(jnp.bfloat16)


def levels(stream_key, extent, shards, least, top_value):
    factor_of = 1.0
    for dim, parts in shards:
        heights = jax.random.uniform(jax.random.fold_in(jax.random.fold_in(stream_key, 6), dim), (parts,), jnp.float32, least / len(shards), top_value / len(shards))
        factor_of = factor_of * jnp.repeat(jnp.exp(heights), extent[dim] // parts).reshape((-1,) + (1,) * (len(extent) - 1 - dim))
    return factor_of


def noise(stream_key, extent, deviation, bound, cuts=(), kind=jnp.bfloat16):
    level = levels(stream_key, extent, cuts, -0.22, 0.18) if cuts else 1.0
    array = jax.random.normal(stream_key, extent, jnp.float32) * deviation * level
    return jnp.minimum(jnp.maximum(array, -bound), bound).astype(kind)


def setup_inputs(seed: int = 0) -> dict:
    key_of = jax.random.split(jax.random.key(seed), 9)
    return {
        "ln_input": noise(key_of[0], (N_SECTION, TOKENS, D), 1.0, 6.0, ((0, 2), (1, 16))),
        "ln_grad": noise(key_of[1], (N_SECTION, TOKENS, D), 1.0, 6.0, ((0, 2), (1, 16))),
        "top_grad": noise(key_of[2], (N_SECTION, TOKENS, D), 1.0, 6.0, ((0, 2), (1, 16))),
        "ln_gain": jnp.clip(1.0 + 0.18 * jax.random.normal(key_of[3], (N_SECTION, D), jnp.float32), 0.1, 1.9),
        "hidden": draw_hidden(jax.random.fold_in(key_of[8], 71), 0),
        "master": noise(key_of[5], (N_SECTION, ROWS, D), 1.0, 6.0, ((0, 2), (1, 16)), jnp.float32),
        "moment": noise(key_of[6], (N_SECTION, ROWS, D), 1.0, 6.0, ((0, 2), (1, 16)), jnp.float32),
        "second": jnp.clip(jnp.exp(math.log(4.0) - 3.6888794 * jax.random.uniform(key_of[7], (N_SECTION, ROWS, D), jnp.float32) ** levels(key_of[7], (N_SECTION, ROWS, D), ((0, 2), (1, 16)), -0.2, 0.2)), 0.1, 4.0),
    }


def layer_back(ln_input, ln_grad, top_grad, ln_gain):
    values = ln_input.astype(jnp.float32)
    row_mean = lax.optimization_barrier(jnp.mean(values, axis=-1, keepdims=True))
    centred = values - row_mean
    inv_std = 1.0 / jnp.sqrt(lax.optimization_barrier(jnp.mean(centred * centred, axis=-1, keepdims=True)) + 1e-05)
    normed = centred * inv_std
    scaled = ln_grad.astype(jnp.float32) * ln_gain
    inner = scaled - lax.optimization_barrier(jnp.mean(scaled, axis=-1, keepdims=True)) - normed * lax.optimization_barrier(jnp.mean(scaled * normed, axis=-1, keepdims=True))
    return (top_grad.astype(jnp.float32) + inner * inv_std).astype(jnp.bfloat16)

def adam_update(grad, master, moment, second):
    new_moment = 0.9 * moment + 0.1 * grad
    new_second = 0.95 * second + 0.05 * grad * grad
    first_fix = 1.0 - 0.9 ** STEP
    second_fix = 1.0 - 0.95 ** STEP
    update = new_moment / first_fix / (jnp.sqrt(new_second / second_fix) + 1e-08)
    new_master = master - 0.05 * (update + 0.1 * master)
    return (new_master, new_moment, new_second)

def reference(ln_input, ln_grad, top_grad, ln_gain, hidden, master, moment, second):
    final_section = N_SECTION - 1

    def one_section(index):
        upper = jnp.minimum(index + 1, final_section)
        passed = layer_back(ln_input[upper], ln_grad[upper], top_grad[upper], ln_gain[upper])
        received = jnp.where(index == final_section, top_grad[index], passed)
        return lax.dot_general(hidden[index], received, (((0,), (0,)), ((), ())), preferred_element_type=jnp.float32)
    grad = lax.map(one_section, jnp.arange(N_SECTION, dtype=jnp.int32))
    new_master, new_moment, new_second = adam_update(grad, master, moment, second)
    weights = new_master.astype(jnp.bfloat16)
    return (new_master, new_moment, new_second, weights)
```

```python
import functools

import jax
import jax.numpy as jnp
from jax import lax
from jax.experimental import pallas as pl
from jax.experimental.pallas import tpu as pltpu
from jax.sharding import PartitionSpec as P

STEP = 20
CORES = 2
CHUNKS = 4
LANES = 128
MESH = pl.DeviceIdType.MESH


def adam_update(grad, master, moment, second):
    new_moment = 0.9 * moment + 0.1 * grad
    new_second = 0.95 * second + 0.05 * grad * grad
    first_fix = 1.0 - 0.9**STEP
    second_fix = 1.0 - 0.95**STEP
    update = new_moment / first_fix / (jnp.sqrt(new_second / second_fix) + 1e-08)
    new_master = master - 0.05 * (update + 0.1 * master)
    return (new_master, new_moment, new_second)


def kernel(
    sections,
    group,
    ln_input_hbm,
    ln_grad_hbm,
    top_grad_hbm,
    gain_hbm,
    hidden_hbm,
    master_hbm,
    moment_hbm,
    second_hbm,
    new_master_ref,
    new_moment_ref,
    new_second_ref,
    weights_ref,
    x_ref,
    g_ref,
    t_ref,
    gain_ref,
    hidden_ref,
    lower_ref,
    state_ref,
    stats_ref,
    mine_ref,
    theirs_ref,
    partner_ref,
    stage_ref,
    recv_ref,
    load_sem,
    state_sem,
    hid_send,
    hid_recv,
    pair_send,
    pair_recv,
    rs_send,
    rs_recv,
    ag_send,
    ag_recv,
    fw_send,
    fw_recv,
):
    tokens, width = x_ref.shape
    rows = hidden_ref.shape[0]
    row_dev = new_master_ref.shape[0]
    chips = group // CORES
    half = rows // CORES
    cols_chunk = width // CHUNKS
    blocks = 4
    block_rows = tokens // blocks

    sec = lax.axis_index("section")
    me = lax.axis_index("dp")
    core = lax.rem(me, CORES)
    chip = lax.div(me, CORES)
    partner = chip * CORES + (1 - core)
    has_lower = sec > 0
    has_upper = sec < sections - 1
    is_last = sec == sections - 1

    def chip_dev(index):
        return index * CORES + core

    def other_chip(step):
        return lax.rem(chip + step, chips)

    barrier = pltpu.get_barrier_semaphore()
    pl.semaphore_signal(barrier, inc=1, device_id=(sec, partner), device_id_type=MESH)
    for step in range(1, chips):
        pl.semaphore_signal(
            barrier, inc=1, device_id=(sec, chip_dev(other_chip(step))), device_id_type=MESH
        )

    @pl.when(has_lower)
    def _():
        for step in range(chips):
            pl.semaphore_signal(
                barrier,
                inc=1,
                device_id=(sec - 1, chip_dev(other_chip(step))),
                device_id_type=MESH,
            )

    @pl.when(has_upper)
    def _():
        for step in range(chips):
            pl.semaphore_signal(
                barrier,
                inc=1,
                device_id=(sec + 1, chip_dev(other_chip(step))),
                device_id_type=MESH,
            )

    def row_block(b):
        return pl.ds(b * block_rows, block_rows)

    x_loads = [
        pltpu.make_async_copy(
            ln_input_hbm.at[row_block(b)], x_ref.at[row_block(b)], load_sem.at[b]
        )
        for b in range(blocks)
    ]
    g_loads = [
        pltpu.make_async_copy(
            ln_grad_hbm.at[row_block(b)], g_ref.at[row_block(b)], load_sem.at[blocks + b]
        )
        for b in range(blocks)
    ]
    t_load = pltpu.make_async_copy(top_grad_hbm, t_ref, load_sem.at[2 * blocks])
    gain_load = pltpu.make_async_copy(gain_hbm, gain_ref, load_sem.at[2 * blocks + 1])
    hidden_load = pltpu.make_async_copy(hidden_hbm, hidden_ref, load_sem.at[2 * blocks + 2])
    state_loads = [
        pltpu.make_async_copy(source, state_ref.at[i], state_sem.at[i])
        for i, source in enumerate((master_hbm, moment_hbm, second_hbm))
    ]
    hidden_copy = pltpu.make_async_remote_copy(
        src_ref=hidden_hbm,
        dst_ref=lower_ref,
        send_sem=hid_send,
        recv_sem=hid_recv,
        device_id=(lax.rem(sec + 1, sections), me),
        device_id_type=MESH,
    )

    @pl.when(has_lower)
    def _():
        gain_load.start()
        for b in range(blocks):
            x_loads[b].start()
            g_loads[b].start()

    @pl.when(has_lower | is_last)
    def _():
        t_load.start()

    @pl.when(is_last)
    def _():
        hidden_load.start()

    for load in state_loads:
        load.start()

    peers = (
        chips
        + jnp.where(has_lower, chips, 0)
        + jnp.where(has_upper, chips, 0)
    )
    pl.semaphore_wait(barrier, peers)

    @pl.when(has_upper)
    def _():
        hidden_copy.start()

    def columns(start, size):
        return pl.ds(pl.multiple_of(start, LANES), size)

    def arranged(source):
        to = lax.broadcasted_iota(jnp.int32, (rows, rows), 0)
        at = lax.broadcasted_iota(jnp.int32, (rows, rows), 1)
        within = lax.rem(to, half)
        which = jnp.where(to < half, core, 1 - core)
        wanted = (lax.div(within, row_dev) * CORES + which) * row_dev + lax.rem(within, row_dev)
        select = jnp.where(at == wanted, 1.0, 0.0).astype(jnp.bfloat16)
        return lax.dot_general(
            select, source[...], (((1,), (0,)), ((), ())), preferred_element_type=jnp.float32
        ).astype(jnp.bfloat16)

    def pair_copy(path, q):
        cols = pl.ds(q * cols_chunk, cols_chunk)
        return pltpu.make_async_remote_copy(
            src_ref=theirs_ref.at[path, :, cols],
            dst_ref=partner_ref.at[path, :, cols],
            send_sem=pair_send.at[path, q],
            recv_sem=pair_recv.at[path, q],
            device_id=(sec, partner),
            device_id_type=MESH,
        )

    def share_copy(path, q, target):
        cols = pl.ds(q * cols_chunk, cols_chunk)
        to_sec = lax.rem(sec + sections - 1, sections) if path == 0 else sec
        return pltpu.make_async_remote_copy(
            src_ref=stage_ref.at[path, target, :, cols],
            dst_ref=recv_ref.at[chip, :, cols],
            send_sem=rs_send.at[path, target, q],
            recv_sem=rs_recv.at[chip, q],
            device_id=(to_sec, chip_dev(target)),
            device_id_type=MESH,
        )

    def own_copy(q):
        cols = pl.ds(q * cols_chunk, cols_chunk)
        return pltpu.make_async_copy(
            stage_ref.at[1, chip, :, cols], recv_ref.at[chip, :, cols], rs_recv.at[chip, q]
        )

    sub = 256

    def product(path, q, lhs, make):
        def body(i, carry):
            cols = columns(q * cols_chunk + i * sub, sub)
            term = jnp.dot(lhs, make(cols), preferred_element_type=jnp.float32)
            mine_ref[path, :, cols] = term[:half]
            theirs_ref[path, :, cols] = term[half:]
            return carry

        lax.fori_loop(0, cols_chunk // sub, body, 0)
        pair_copy(path, q).start()

    def reduce_send(path, q):
        pair_copy(path, q).wait_recv()
        part = 512

        def body(i, carry):
            cols = columns(q * cols_chunk + i * part, part)
            total = (mine_ref[path, :, cols] + partner_ref[path, :, cols]).astype(jnp.bfloat16)
            for k in range(chips):
                stage_ref[path, k, :, cols] = total[k * row_dev : (k + 1) * row_dev]
            return carry

        lax.fori_loop(0, cols_chunk // part, body, 0)
        if path == 1:
            own_copy(q).start()
        for step in range(1 if path == 1 else 0, chips):
            share_copy(path, q, other_chip(step)).start()

    @pl.when(has_lower)
    def _():
        gain_load.wait()
        sub_rows = 16
        span = 1536

        def fold(value):
            parts = [value[:, i * LANES : (i + 1) * LANES] for i in range(span // LANES)]
            while len(parts) > 1:
                parts = [
                    parts[i] + parts[i + 1] if i + 1 < len(parts) else parts[i]
                    for i in range(0, len(parts), 2)
                ]
            return parts[0]

        def statistics(r, carry):
            at = pl.ds(pl.multiple_of(r * sub_rows, sub_rows), sub_rows)
            zero = jnp.zeros((sub_rows, LANES), jnp.float32)

            def first(i, sums):
                cols = columns(i * span, span)
                values = x_ref[at, cols].astype(jnp.float32)
                scaled = g_ref[at, cols].astype(jnp.float32) * gain_ref[:, cols]
                return (sums[0] + fold(values), sums[1] + fold(scaled))

            sums = lax.fori_loop(0, width // span, first, (zero, zero))
            mean = jnp.sum(sums[0], axis=-1, keepdims=True) / width
            mean_scaled = jnp.sum(sums[1], axis=-1, keepdims=True) / width

            def second(i, sums):
                cols = columns(i * span, span)
                centred = x_ref[at, cols].astype(jnp.float32) - mean
                scaled = g_ref[at, cols].astype(jnp.float32) * gain_ref[:, cols]
                return (sums[0] + fold(centred * centred), sums[1] + fold(scaled * centred))

            sums = lax.fori_loop(0, width // span, second, (zero, zero))
            var = jnp.sum(sums[0], axis=-1, keepdims=True) / width
            inv_std = 1.0 / jnp.sqrt(var + 1e-05)
            along = jnp.sum(sums[1], axis=-1, keepdims=True) / width * inv_std
            full = (sub_rows, LANES)
            stats_ref[0, at, :] = jnp.broadcast_to(mean, full)
            stats_ref[1, at, :] = jnp.broadcast_to(mean_scaled, full)
            stats_ref[2, at, :] = jnp.broadcast_to(along * inv_std, full)
            stats_ref[3, at, :] = jnp.broadcast_to(inv_std, full)
            return carry

        per_block = block_rows // sub_rows
        for b in range(blocks):
            x_loads[b].wait()
            g_loads[b].wait()
            lax.fori_loop(b * per_block, (b + 1) * per_block, statistics, 0)

    @pl.when(has_lower | is_last)
    def _():
        t_load.wait()

    @pl.when(has_lower)
    def _():
        hidden_copy.wait_recv()
        lhs = arranged(lower_ref)

        def passed(cols):
            def wide(i):
                return jnp.concatenate([stats_ref[i]] * (sub // LANES), axis=1)

            centred = x_ref[:, cols].astype(jnp.float32) - wide(0)
            scaled = g_ref[:, cols].astype(jnp.float32) * gain_ref[:, cols]
            inner = (scaled - wide(1)) - centred * wide(2)
            return (t_ref[:, cols].astype(jnp.float32) + inner * wide(3)).astype(jnp.bfloat16)

        for q in range(CHUNKS):
            product(0, q, lhs, passed)
            if q:
                reduce_send(0, q - 1)
        reduce_send(0, CHUNKS - 1)

    @pl.when(is_last)
    def _():
        hidden_load.wait()
        lhs = arranged(hidden_ref)
        for q in range(CHUNKS):
            product(1, q, lhs, lambda cols: t_ref[:, cols])
            if q:
                reduce_send(1, q - 1)
        reduce_send(1, CHUNKS - 1)

    def gather_copy(q, source, target):
        cols = pl.ds(q * cols_chunk, cols_chunk)
        return pltpu.make_async_remote_copy(
            src_ref=weights_ref.at[chip_dev(source), :, cols],
            dst_ref=weights_ref.at[chip_dev(source), :, cols],
            send_sem=ag_send.at[target, q],
            recv_sem=ag_recv.at[source, q],
            device_id=(sec, chip_dev(target)),
            device_id_type=MESH,
        )

    def forward_copy(q, source):
        cols = pl.ds(q * cols_chunk, cols_chunk)
        return pltpu.make_async_remote_copy(
            src_ref=weights_ref.at[chip_dev(source), :, cols],
            dst_ref=weights_ref.at[chip_dev(source), :, cols],
            send_sem=fw_send.at[source, q],
            recv_sem=fw_recv.at[source, q],
            device_id=(sec, partner),
            device_id_type=MESH,
        )

    for load in state_loads:
        load.wait()

    for q in range(CHUNKS):
        cols = pl.ds(q * cols_chunk, cols_chunk)
        for k in range(chips):
            pltpu.make_async_copy(
                recv_ref.at[k, :, cols], recv_ref.at[k, :, cols], rs_recv.at[k, q]
            ).wait()
        part = 512

        def update(i, carry):
            at = columns(q * cols_chunk + i * part, part)
            grad = jnp.sum(recv_ref[:, :, at].astype(jnp.float32), axis=0)
            masters, moments, seconds = adam_update(
                grad, state_ref[0, :, at], state_ref[1, :, at], state_ref[2, :, at]
            )
            new_master_ref[:, at] = masters
            new_moment_ref[:, at] = moments
            new_second_ref[:, at] = seconds
            weights_ref[me, :, at] = masters.astype(jnp.bfloat16)
            return carry

        lax.fori_loop(0, cols_chunk // part, update, 0)
        for step in range(1, chips):
            gather_copy(q, chip, other_chip(step)).start()
        forward_copy(q, chip).start()

    for q in range(CHUNKS):
        for step in range(1, chips):
            source = other_chip(step)
            gather_copy(q, source, chip).wait_recv()
            forward_copy(q, source).start()

    for q in range(CHUNKS):
        for step in range(chips):
            source = other_chip(step)
            forward_copy(q, source).wait()
            if step:
                gather_copy(q, chip, source).wait_send()

    def finish(path):
        for q in range(CHUNKS):
            pair_copy(path, q).wait_send()
            for step in range(1 if path == 1 else 0, chips):
                share_copy(path, q, other_chip(step)).wait_send()

    @pl.when(has_lower)
    def _():
        finish(0)

    @pl.when(is_last)
    def _():
        finish(1)

    @pl.when(has_upper)
    def _():
        hidden_copy.wait_send()


def solution(mesh):
    sections = mesh.shape["section"]
    group = mesh.shape["dp"]
    chips = group // CORES

    def step(ln_input, ln_grad, top_grad, ln_gain, hidden, master, moment, second):
        tokens, width = ln_input.shape[1:]
        rows = hidden.shape[2]
        row_dev = master.shape[1]
        half = rows // CORES
        any_space = pl.BlockSpec(memory_space=pl.ANY)
        vmem = pl.BlockSpec(memory_space=pltpu.VMEM)
        state = jax.ShapeDtypeStruct((row_dev, width), jnp.float32)
        dma = pltpu.SemaphoreType.DMA
        outs = pl.pallas_call(
            functools.partial(kernel, sections, group),
            out_shape=(
                state,
                state,
                state,
                jax.ShapeDtypeStruct((group, row_dev, width), jnp.bfloat16),
            ),
            in_specs=[any_space] * 8,
            out_specs=(vmem,) * 4,
            scratch_shapes=[
                pltpu.VMEM((tokens, width), jnp.bfloat16),
                pltpu.VMEM((tokens, width), jnp.bfloat16),
                pltpu.VMEM((tokens, width), jnp.bfloat16),
                pltpu.VMEM((1, width), jnp.float32),
                pltpu.VMEM((rows, tokens), jnp.bfloat16),
                pltpu.VMEM((rows, tokens), jnp.bfloat16),
                pltpu.VMEM((3, row_dev, width), jnp.float32),
                pltpu.VMEM((4, tokens, LANES), jnp.float32),
                pltpu.VMEM((2, half, width), jnp.float32),
                pltpu.VMEM((2, half, width), jnp.float32),
                pltpu.VMEM((2, half, width), jnp.float32),
                pltpu.VMEM((2, chips, row_dev, width), jnp.bfloat16),
                pltpu.VMEM((chips, row_dev, width), jnp.bfloat16),
                dma((11,)),
                dma((3,)),
                dma,
                dma,
                dma((2, CHUNKS)),
                dma((2, CHUNKS)),
                dma((2, chips, CHUNKS)),
                dma((chips, CHUNKS)),
                dma((chips, CHUNKS)),
                dma((chips, CHUNKS)),
                dma((chips, CHUNKS)),
                dma((chips, CHUNKS)),
            ],
            compiler_params=pltpu.CompilerParams(
                collective_id=0, has_side_effects=True, vmem_limit_bytes=60 * 2**20
            ),
        )(
            ln_input[0],
            ln_grad[0],
            top_grad[0],
            ln_gain,
            hidden[0].T,
            master[0],
            moment[0],
            second[0],
        )
        masters, moments, seconds, gathered = outs
        weights = gathered.reshape(rows, width)
        return (masters[None], moments[None], seconds[None], weights[None])

    return jax.shard_map(
        step,
        mesh=mesh,
        in_specs=(
            P("section", "dp", None),
            P("section", "dp", None),
            P("section", "dp", None),
            P("section", None),
            P("section", "dp", None),
            P("section", "dp", None),
            P("section", "dp", None),
            P("section", "dp", None),
        ),
        out_specs=(
            P("section", "dp", None),
            P("section", "dp", None),
            P("section", "dp", None),
            P("section", None, None),
        ),
        check_vma=False,
    )
```

```python
import functools

import jax
import jax.numpy as jnp
from jax import lax
from jax.experimental import pallas as pl
from jax.experimental.pallas import tpu as pltpu
from jax.sharding import PartitionSpec as P

STEP = 20
CORES = 2
CHUNKS = 4
LANES = 128
MESH = pl.DeviceIdType.MESH


def adam_update(grad, master, moment, second):
    new_moment = 0.9 * moment + 0.1 * grad
    new_second = 0.95 * second + 0.05 * grad * grad
    first_fix = 1.0 - 0.9**STEP
    second_fix = 1.0 - 0.95**STEP
    update = new_moment / first_fix / (jnp.sqrt(new_second / second_fix) + 1e-08)
    new_master = master - 0.05 * (update + 0.1 * master)
    return (new_master, new_moment, new_second)


def kernel(
    sections,
    group,
    inner,
    ln_input_hbm,
    ln_grad_hbm,
    top_grad_hbm,
    gain_hbm,
    hidden_hbm,
    master_hbm,
    moment_hbm,
    second_hbm,
    new_master_ref,
    new_moment_ref,
    new_second_ref,
    weights_ref,
    x_ref,
    g_ref,
    t_ref,
    gain_ref,
    hidden_ref,
    lower_ref,
    state_ref,
    stats_ref,
    mine_ref,
    theirs_ref,
    partner_ref,
    stage_ref,
    recv_ref,
    load_sem,
    state_sem,
    hid_send,
    hid_recv,
    pair_send,
    pair_recv,
    rs_send,
    rs_recv,
    ag_send,
    ag_recv,
    fw_send,
    fw_recv,
):
    tokens, width = x_ref.shape
    rows = hidden_ref.shape[0]
    row_dev = new_master_ref.shape[0]
    chips = group // CORES
    half = rows // CORES
    cols_chunk = width // CHUNKS
    blocks = 4
    block_rows = tokens // blocks

    sec = lax.axis_index("section")
    me = lax.axis_index("dp")
    core = lax.rem(me, CORES)
    chip = lax.div(me, CORES)
    partner = chip * CORES + (1 - core)
    has_lower = sec > 0
    has_upper = sec < sections - 1
    is_last = sec == sections - 1

    def chip_dev(index):
        return index * CORES + core

    def other_chip(step):
        return lax.rem(chip + step, chips)

    barrier = pltpu.get_barrier_semaphore()
    pl.semaphore_signal(barrier, inc=1, device_id=(sec, partner), device_id_type=MESH)
    for step in range(1, chips):
        pl.semaphore_signal(
            barrier, inc=1, device_id=(sec, chip_dev(other_chip(step))), device_id_type=MESH
        )

    @pl.when(has_lower)
    def _():
        for step in range(chips):
            pl.semaphore_signal(
                barrier,
                inc=1,
                device_id=(sec - 1, chip_dev(other_chip(step))),
                device_id_type=MESH,
            )

    @pl.when(has_upper)
    def _():
        for step in range(chips):
            pl.semaphore_signal(
                barrier,
                inc=1,
                device_id=(sec + 1, chip_dev(other_chip(step))),
                device_id_type=MESH,
            )

    def row_block(b):
        return pl.ds(b * block_rows, block_rows)

    x_loads = [
        pltpu.make_async_copy(
            ln_input_hbm.at[row_block(b)], x_ref.at[row_block(b)], load_sem.at[b]
        )
        for b in range(blocks)
    ]
    g_loads = [
        pltpu.make_async_copy(
            ln_grad_hbm.at[row_block(b)], g_ref.at[row_block(b)], load_sem.at[blocks + b]
        )
        for b in range(blocks)
    ]
    t_load = pltpu.make_async_copy(top_grad_hbm, t_ref, load_sem.at[2 * blocks])
    gain_load = pltpu.make_async_copy(gain_hbm, gain_ref, load_sem.at[2 * blocks + 1])
    hidden_load = pltpu.make_async_copy(hidden_hbm, hidden_ref, load_sem.at[2 * blocks + 2])
    state_loads = [
        pltpu.make_async_copy(source, state_ref.at[i], state_sem.at[i])
        for i, source in enumerate((master_hbm, moment_hbm, second_hbm))
    ]
    hidden_copy = pltpu.make_async_remote_copy(
        src_ref=hidden_hbm,
        dst_ref=lower_ref,
        send_sem=hid_send,
        recv_sem=hid_recv,
        device_id=(lax.rem(sec + 1, sections), me),
        device_id_type=MESH,
    )

    @pl.when(is_last)
    def _():
        hidden_load.start()

    @pl.when(has_lower | is_last)
    def _():
        t_load.start()

    @pl.when(has_lower)
    def _():
        gain_load.start()
        for b in range(blocks):
            x_loads[b].start()
            g_loads[b].start()

    for load in state_loads:
        load.start()

    peers = (
        chips
        + jnp.where(has_lower, chips, 0)
        + jnp.where(has_upper, chips, 0)
    )
    pl.semaphore_wait(barrier, peers)

    @pl.when(has_upper)
    def _():
        hidden_copy.start()

    def columns(start, size):
        return pl.ds(pl.multiple_of(start, LANES), size)

    def arranged(source):
        to = lax.broadcasted_iota(jnp.int32, (rows, rows), 0)
        at = lax.broadcasted_iota(jnp.int32, (rows, rows), 1)
        within = lax.rem(to, half)
        which = jnp.where(to < half, core, 1 - core)
        wanted = (lax.div(within, row_dev) * CORES + which) * row_dev + lax.rem(within, row_dev)
        select = jnp.where(at == wanted, 1.0, 0.0).astype(jnp.bfloat16)
        return lax.dot_general(
            select, source[...], (((1,), (0,)), ((), ())), preferred_element_type=jnp.float32
        ).astype(jnp.bfloat16)

    def pair_copy(path, q):
        cols = pl.ds(q * cols_chunk, cols_chunk)
        return pltpu.make_async_remote_copy(
            src_ref=theirs_ref.at[path, :, cols],
            dst_ref=partner_ref.at[path, :, cols],
            send_sem=pair_send.at[path, q],
            recv_sem=pair_recv.at[path, q],
            device_id=(sec, partner),
            device_id_type=MESH,
        )

    def share_copy(path, q, target):
        cols = pl.ds(q * cols_chunk, cols_chunk)
        to_sec = lax.rem(sec + sections - 1, sections) if path == 0 else sec
        return pltpu.make_async_remote_copy(
            src_ref=stage_ref.at[path, target, :, cols],
            dst_ref=recv_ref.at[chip, :, cols],
            send_sem=rs_send.at[path, target, q],
            recv_sem=rs_recv.at[chip, q],
            device_id=(to_sec, chip_dev(target)),
            device_id_type=MESH,
        )

    def own_copy(q):
        cols = pl.ds(q * cols_chunk, cols_chunk)
        return pltpu.make_async_copy(
            stage_ref.at[1, chip, :, cols], recv_ref.at[chip, :, cols], rs_recv.at[chip, q]
        )

    sub = 256

    def product(path, q, lhs, make):
        def body(i, carry):
            cols = columns(q * cols_chunk + i * sub, sub)
            term = jnp.dot(lhs, make(cols), preferred_element_type=jnp.float32)
            mine_ref[path, :, cols] = term[:half]
            theirs_ref[path, :, cols] = term[half:]
            return carry

        lax.fori_loop(0, cols_chunk // sub, body, 0)
        pair_copy(path, q).start()

    def reduce_send(path, q):
        pair_copy(path, q).wait_recv()
        part = 512

        def body(i, carry):
            cols = columns(q * cols_chunk + i * part, part)
            total = (mine_ref[path, :, cols] + partner_ref[path, :, cols]).astype(jnp.bfloat16)
            for k in range(chips):
                stage_ref[path, k, :, cols] = total[k * row_dev : (k + 1) * row_dev]
            return carry

        lax.fori_loop(0, cols_chunk // part, body, 0)
        if path == 1:
            own_copy(q).start()
        for step in range(1 if path == 1 else 0, chips):
            share_copy(path, q, other_chip(step)).start()

    @pl.when(has_lower | is_last)
    def _():
        t_load.wait()

    @pl.when(is_last)
    def _():
        hidden_load.wait()
        lhs = arranged(hidden_ref)
        for q in range(CHUNKS):
            product(1, q, lhs, lambda cols: t_ref[:, cols])
            if q:
                reduce_send(1, q - 1)

    def statistics_of(first_block, last_block):
        sub_rows = 16
        span = 1536

        def fold(value):
            parts = [value[:, i * LANES : (i + 1) * LANES] for i in range(span // LANES)]
            while len(parts) > 1:
                parts = [
                    parts[i] + parts[i + 1] if i + 1 < len(parts) else parts[i]
                    for i in range(0, len(parts), 2)
                ]
            return parts[0]

        def statistics(r, carry):
            at = pl.ds(pl.multiple_of(r * sub_rows, sub_rows), sub_rows)
            zero = jnp.zeros((sub_rows, LANES), jnp.float32)

            def first(i, sums):
                cols = columns(i * span, span)
                values = x_ref[at, cols].astype(jnp.float32)
                scaled = g_ref[at, cols].astype(jnp.float32) * gain_ref[:, cols]
                return (sums[0] + fold(values), sums[1] + fold(scaled))

            sums = lax.fori_loop(0, width // span, first, (zero, zero))
            mean = jnp.sum(sums[0], axis=-1, keepdims=True) / width
            mean_scaled = jnp.sum(sums[1], axis=-1, keepdims=True) / width

            def second(i, sums):
                cols = columns(i * span, span)
                centred = x_ref[at, cols].astype(jnp.float32) - mean
                scaled = g_ref[at, cols].astype(jnp.float32) * gain_ref[:, cols]
                return (sums[0] + fold(centred * centred), sums[1] + fold(scaled * centred))

            sums = lax.fori_loop(0, width // span, second, (zero, zero))
            var = jnp.sum(sums[0], axis=-1, keepdims=True) / width
            inv_std = 1.0 / jnp.sqrt(var + 1e-05)
            along = jnp.sum(sums[1], axis=-1, keepdims=True) / width * inv_std
            full = (sub_rows, LANES)
            stats_ref[0, at, :] = jnp.broadcast_to(mean, full)
            stats_ref[1, at, :] = jnp.broadcast_to(mean_scaled, full)
            stats_ref[2, at, :] = jnp.broadcast_to(along * inv_std, full)
            stats_ref[3, at, :] = jnp.broadcast_to(inv_std, full)
            return carry

        per_block = block_rows // sub_rows
        for b in range(first_block, last_block):
            x_loads[b].wait()
            g_loads[b].wait()
            lax.fori_loop(b * per_block, (b + 1) * per_block, statistics, 0)

    @pl.when(has_lower)
    def _():
        gain_load.wait()
        statistics_of(0, 1)

    @pl.when(is_last)
    def _():
        reduce_send(1, CHUNKS - 1)

    @pl.when(has_lower)
    def _():
        statistics_of(1, blocks)

    @pl.when(has_lower)
    def _():
        hidden_copy.wait_recv()
        lhs = arranged(lower_ref)

        def passed(cols):
            def wide(i):
                return jnp.concatenate([stats_ref[i]] * (sub // LANES), axis=1)

            centred = x_ref[:, cols].astype(jnp.float32) - wide(0)
            scaled = g_ref[:, cols].astype(jnp.float32) * gain_ref[:, cols]
            inner = (scaled - wide(1)) - centred * wide(2)
            return (t_ref[:, cols].astype(jnp.float32) + inner * wide(3)).astype(jnp.bfloat16)

        for q in range(CHUNKS):
            product(0, q, lhs, passed)
            if q:
                reduce_send(0, q - 1)
        reduce_send(0, CHUNKS - 1)

    def gather_copy(q, source, target):
        cols = pl.ds(q * cols_chunk, cols_chunk)
        return pltpu.make_async_remote_copy(
            src_ref=weights_ref.at[chip_dev(source), :, cols],
            dst_ref=weights_ref.at[chip_dev(source), :, cols],
            send_sem=ag_send.at[lax.div(source, inner), target, q],
            recv_sem=ag_recv.at[source, q],
            device_id=(sec, chip_dev(target)),
            device_id_type=MESH,
        )

    def forward_copy(q, source):
        cols = pl.ds(q * cols_chunk, cols_chunk)
        return pltpu.make_async_remote_copy(
            src_ref=weights_ref.at[chip_dev(source), :, cols],
            dst_ref=weights_ref.at[chip_dev(source), :, cols],
            send_sem=fw_send.at[source, q],
            recv_sem=fw_recv.at[source, q],
            device_id=(sec, partner),
            device_id_type=MESH,
        )

    outer = chips // inner
    my_outer = lax.div(chip, inner)
    my_inner = lax.rem(chip, inner)

    def at_chip(outer_step, inner_step):
        return (
            lax.rem(my_outer + outer_step, outer) * inner
            + lax.rem(my_inner + inner_step, inner)
        )

    for load in state_loads:
        load.wait()

    for q in range(CHUNKS):
        cols = pl.ds(q * cols_chunk, cols_chunk)
        for k in range(chips):
            pltpu.make_async_copy(
                recv_ref.at[k, :, cols], recv_ref.at[k, :, cols], rs_recv.at[k, q]
            ).wait()
        part = 512

        def update(i, carry):
            at = columns(q * cols_chunk + i * part, part)
            grad = jnp.sum(recv_ref[:, :, at].astype(jnp.float32), axis=0)
            masters, moments, seconds = adam_update(
                grad, state_ref[0, :, at], state_ref[1, :, at], state_ref[2, :, at]
            )
            new_master_ref[:, at] = masters
            new_moment_ref[:, at] = moments
            new_second_ref[:, at] = seconds
            weights_ref[me, :, at] = masters.astype(jnp.bfloat16)
            return carry

        lax.fori_loop(0, cols_chunk // part, update, 0)
        for step in range(1, outer):
            gather_copy(q, chip, at_chip(step, 0)).start()
        for step in range(1, inner):
            gather_copy(q, chip, at_chip(0, step)).start()
        forward_copy(q, chip).start()

    for q in range(CHUNKS):
        for outer_step in range(1, outer):
            source = at_chip(outer_step, 0)
            gather_copy(q, source, chip).wait_recv()
            for step in range(1, inner):
                gather_copy(q, source, at_chip(0, step)).start()
            forward_copy(q, source).start()
    for q in range(CHUNKS):
        for outer_step in range(outer):
            for step in range(1, inner):
                source = at_chip(outer_step, step)
                gather_copy(q, source, chip).wait_recv()
                forward_copy(q, source).start()

    for q in range(CHUNKS):
        for outer_step in range(outer):
            for step in range(inner):
                forward_copy(q, at_chip(outer_step, step)).wait()
            for step in range(1, inner):
                gather_copy(q, at_chip(outer_step, 0), at_chip(0, step)).wait_send()
            if outer_step:
                gather_copy(q, chip, at_chip(outer_step, 0)).wait_send()

    def finish(path):
        for q in range(CHUNKS):
            pair_copy(path, q).wait_send()
            for step in range(1 if path == 1 else 0, chips):
                share_copy(path, q, other_chip(step)).wait_send()

    @pl.when(has_lower)
    def _():
        finish(0)

    @pl.when(is_last)
    def _():
        finish(1)

    @pl.when(has_upper)
    def _():
        hidden_copy.wait_send()


def write_out(master, moment, second, gathered, new_master, new_moment, new_second, weights):
    new_master[...] = master[...]
    new_moment[...] = moment[...]
    new_second[...] = second[...]
    group, row_dev, _ = gathered.shape
    for owner in range(group):
        weights[owner * row_dev : (owner + 1) * row_dev] = gathered[owner]


def solution(mesh):
    sections = mesh.shape["section"]
    group = mesh.shape["dp"]
    chips = group // CORES
    inner = 1
    while inner * inner * 4 <= chips and chips % (inner * 2) == 0:
        inner *= 2

    def step(ln_input, ln_grad, top_grad, ln_gain, hidden, master, moment, second):
        tokens, width = ln_input.shape[1:]
        rows = hidden.shape[2]
        row_dev = master.shape[1]
        half = rows // CORES
        any_space = pl.BlockSpec(memory_space=pl.ANY)
        vmem = pl.BlockSpec(memory_space=pltpu.VMEM)
        state = jax.ShapeDtypeStruct((row_dev, width), jnp.float32)
        dma = pltpu.SemaphoreType.DMA
        outs = pl.pallas_call(
            functools.partial(kernel, sections, group, inner),
            out_shape=(
                state,
                state,
                state,
                jax.ShapeDtypeStruct((group, row_dev, width), jnp.bfloat16),
            ),
            in_specs=[any_space] * 8,
            out_specs=(vmem,) * 4,
            scratch_shapes=[
                pltpu.VMEM((tokens, width), jnp.bfloat16),
                pltpu.VMEM((tokens, width), jnp.bfloat16),
                pltpu.VMEM((tokens, width), jnp.bfloat16),
                pltpu.VMEM((1, width), jnp.float32),
                pltpu.VMEM((rows, tokens), jnp.bfloat16),
                pltpu.VMEM((rows, tokens), jnp.bfloat16),
                pltpu.VMEM((3, row_dev, width), jnp.float32),
                pltpu.VMEM((4, tokens, LANES), jnp.float32),
                pltpu.VMEM((2, half, width), jnp.float32),
                pltpu.VMEM((2, half, width), jnp.float32),
                pltpu.VMEM((2, half, width), jnp.float32),
                pltpu.VMEM((2, chips, row_dev, width), jnp.bfloat16),
                pltpu.VMEM((chips, row_dev, width), jnp.bfloat16),
                dma((11,)),
                dma((3,)),
                dma,
                dma,
                dma((2, CHUNKS)),
                dma((2, CHUNKS)),
                dma((2, chips, CHUNKS)),
                dma((chips, CHUNKS)),
                dma((chips // inner, chips, CHUNKS)),
                dma((chips, CHUNKS)),
                dma((chips, CHUNKS)),
                dma((chips, CHUNKS)),
            ],
            compiler_params=pltpu.CompilerParams(
                collective_id=0, has_side_effects=True, vmem_limit_bytes=60 * 2**20
            ),
        )(
            ln_input[0],
            ln_grad[0],
            top_grad[0],
            ln_gain,
            hidden[0].T,
            master[0],
            moment[0],
            second[0],
        )
        slab = width // 4
        strip = pl.BlockSpec((row_dev, slab), lambda i: (0, i))
        masters, moments, seconds, weights = pl.pallas_call(
            write_out,
            grid=(width // slab,),
            out_shape=(state, state, state, jax.ShapeDtypeStruct((rows, width), jnp.bfloat16)),
            in_specs=[strip] * 3 + [pl.BlockSpec((group, row_dev, slab), lambda i: (0, 0, i))],
            out_specs=(strip,) * 3 + (pl.BlockSpec((rows, slab), lambda i: (0, i)),),
        )(*outs)
        return (masters[None], moments[None], seconds[None], weights[None])

    return jax.shard_map(
        step,
        mesh=mesh,
        in_specs=(
            P("section", "dp", None),
            P("section", "dp", None),
            P("section", "dp", None),
            P("section", None),
            P("section", "dp", None),
            P("section", "dp", None),
            P("section", "dp", None),
            P("section", "dp", None),
        ),
        out_specs=(
            P("section", "dp", None),
            P("section", "dp", None),
            P("section", "dp", None),
            P("section", None, None),
        ),
        check_vma=False,
    )
```

```python
import functools

import jax
import jax.numpy as jnp
from jax import lax
from jax.experimental import pallas as pl
from jax.experimental.pallas import tpu as pltpu
from jax.sharding import PartitionSpec as P

STEP = 20
CORES = 2
CHUNKS = 4
LANES = 128
MESH = pl.DeviceIdType.MESH


def adam_update(grad, master, moment, second):
    new_moment = 0.9 * moment + 0.1 * grad
    new_second = 0.95 * second + 0.05 * grad * grad
    first_fix = 1.0 - 0.9**STEP
    second_fix = 1.0 - 0.95**STEP
    update = new_moment / first_fix / (jnp.sqrt(new_second / second_fix) + 1e-08)
    new_master = master - 0.05 * (update + 0.1 * master)
    return (new_master, new_moment, new_second)


def kernel(
    sections,
    group,
    inner,
    ln_input_hbm,
    ln_grad_hbm,
    top_grad_hbm,
    gain_hbm,
    hidden_hbm,
    master_hbm,
    moment_hbm,
    second_hbm,
    new_master_ref,
    new_moment_ref,
    new_second_ref,
    weights_ref,
    x_ref,
    g_ref,
    t_ref,
    passed_ref,
    gain_ref,
    hidden_ref,
    lower_ref,
    state_ref,
    stats_ref,
    mine_ref,
    theirs_ref,
    partner_ref,
    stage_ref,
    base_ref,
    side_ref,
    part_ref,
    recv_ref,
    load_sem,
    state_sem,
    hid_send,
    hid_recv,
    pair_send,
    pair_recv,
    down_send,
    down_recv,
    inner_send,
    inner_recv,
    outer_send,
    outer_recv,
    ag_send,
    ag_recv,
    fw_send,
    fw_recv,
):
    tokens, width = x_ref.shape
    rows = hidden_ref.shape[0]
    row_dev = new_master_ref.shape[0]
    chips = group // CORES
    half = rows // CORES
    cols_chunk = width // CHUNKS
    blocks = 4
    block_rows = tokens // blocks

    sec = lax.axis_index("section")
    me = lax.axis_index("dp")
    core = lax.rem(me, CORES)
    chip = lax.div(me, CORES)
    partner = chip * CORES + (1 - core)
    has_lower = sec > 0
    has_upper = sec < sections - 1
    is_last = sec == sections - 1

    def chip_dev(index):
        return index * CORES + core

    outer = chips // inner
    my_outer = lax.div(chip, inner)
    my_inner = lax.rem(chip, inner)

    def at_chip(outer_step, inner_step):
        return (
            lax.rem(my_outer + outer_step, outer) * inner
            + lax.rem(my_inner + inner_step, inner)
        )

    barrier = pltpu.get_barrier_semaphore()
    pl.semaphore_signal(barrier, inc=1, device_id=(sec, partner), device_id_type=MESH)
    for step in range(1, outer):
        pl.semaphore_signal(
            barrier, inc=1, device_id=(sec, chip_dev(at_chip(step, 0))), device_id_type=MESH
        )
    for step in range(1, inner):
        pl.semaphore_signal(
            barrier, inc=1, device_id=(sec, chip_dev(at_chip(0, step))), device_id_type=MESH
        )

    @pl.when(has_lower)
    def _():
        pl.semaphore_signal(barrier, inc=1, device_id=(sec - 1, me), device_id_type=MESH)

    @pl.when(has_upper)
    def _():
        pl.semaphore_signal(barrier, inc=1, device_id=(sec + 1, me), device_id_type=MESH)

    def row_block(b):
        return pl.ds(b * block_rows, block_rows)

    x_loads = [
        pltpu.make_async_copy(
            ln_input_hbm.at[row_block(b)], x_ref.at[row_block(b)], load_sem.at[b]
        )
        for b in range(blocks)
    ]
    g_loads = [
        pltpu.make_async_copy(
            ln_grad_hbm.at[row_block(b)], g_ref.at[row_block(b)], load_sem.at[blocks + b]
        )
        for b in range(blocks)
    ]
    t_load = pltpu.make_async_copy(top_grad_hbm, t_ref, load_sem.at[2 * blocks])
    gain_load = pltpu.make_async_copy(gain_hbm, gain_ref, load_sem.at[2 * blocks + 1])
    hidden_load = pltpu.make_async_copy(hidden_hbm, hidden_ref, load_sem.at[2 * blocks + 2])
    state_loads = [
        pltpu.make_async_copy(source, state_ref.at[i], state_sem.at[i])
        for i, source in enumerate((master_hbm, moment_hbm, second_hbm))
    ]
    hidden_copy = pltpu.make_async_remote_copy(
        src_ref=hidden_hbm,
        dst_ref=lower_ref,
        send_sem=hid_send,
        recv_sem=hid_recv,
        device_id=(lax.rem(sec + 1, sections), me),
        device_id_type=MESH,
    )

    @pl.when(is_last)
    def _():
        hidden_load.start()

    @pl.when(has_lower)
    def _():
        gain_load.start()
        for b in range(blocks):
            x_loads[b].start()
            g_loads[b].start()

    @pl.when(has_lower | is_last)
    def _():
        t_load.start()

    for load in state_loads:
        load.start()

    peers = (
        outer
        + inner
        - 1
        + jnp.where(has_lower, 1, 0)
        + jnp.where(has_upper, 1, 0)
    )
    pl.semaphore_wait(barrier, peers)

    @pl.when(has_upper)
    def _():
        hidden_copy.start()

    def columns(start, size):
        return pl.ds(pl.multiple_of(start, LANES), size)

    def arranged(source):
        to = lax.broadcasted_iota(jnp.int32, (rows, rows), 0)
        at = lax.broadcasted_iota(jnp.int32, (rows, rows), 1)
        within = lax.rem(to, half)
        which = jnp.where(to < half, core, 1 - core)
        place = lax.div(within, row_dev)
        owner = lax.rem(place, outer) * inner + lax.div(place, outer)
        wanted = (owner * CORES + which) * row_dev + lax.rem(within, row_dev)
        select = jnp.where(at == wanted, 1.0, 0.0).astype(jnp.bfloat16)
        return lax.dot_general(
            select, source[...], (((1,), (0,)), ((), ())), preferred_element_type=jnp.float32
        ).astype(jnp.bfloat16)

    def pair_copy(path, q):
        cols = pl.ds(q * cols_chunk, cols_chunk)
        return pltpu.make_async_remote_copy(
            src_ref=theirs_ref.at[path, :, cols],
            dst_ref=partner_ref.at[path, :, cols],
            send_sem=pair_send.at[path, q],
            recv_sem=pair_recv.at[path, q],
            device_id=(sec, partner),
            device_id_type=MESH,
        )

    def down_copy(q):
        cols = pl.ds(q * cols_chunk, cols_chunk)
        return pltpu.make_async_remote_copy(
            src_ref=stage_ref.at[:, :, cols],
            dst_ref=base_ref.at[:, :, cols],
            send_sem=down_send.at[q],
            recv_sem=down_recv.at[q],
            device_id=(lax.rem(sec + sections - 1, sections), me),
            device_id_type=MESH,
        )

    def inner_copy(q, source, step):
        cols = pl.ds(q * cols_chunk, cols_chunk)
        target = lax.rem(my_inner + step, inner)
        return pltpu.make_async_remote_copy(
            src_ref=base_ref.at[pl.ds(target * outer, outer), :, cols],
            dst_ref=side_ref.at[source, :, :, cols],
            send_sem=inner_send.at[target, q],
            recv_sem=inner_recv.at[source, q],
            device_id=(sec, chip_dev(at_chip(0, step))),
            device_id_type=MESH,
        )

    def outer_copy(q, source, step):
        cols = pl.ds(q * cols_chunk, cols_chunk)
        target = lax.rem(my_outer + step, outer)
        return pltpu.make_async_remote_copy(
            src_ref=part_ref.at[target, :, cols],
            dst_ref=recv_ref.at[source, :, cols],
            send_sem=outer_send.at[target, q],
            recv_sem=outer_recv.at[source, q],
            device_id=(sec, chip_dev(at_chip(step, 0))),
            device_id_type=MESH,
        )

    def own_copy(q):
        cols = pl.ds(q * cols_chunk, cols_chunk)
        return pltpu.make_async_copy(
            part_ref.at[my_outer, :, cols],
            recv_ref.at[my_outer, :, cols],
            outer_recv.at[my_outer, q],
        )

    def send_inner(q):
        for step in range(1, inner):
            inner_copy(q, my_inner, step).start()

    def add_inner(q):
        for step in range(1, inner):
            inner_copy(q, lax.rem(my_inner + step, inner), step).wait_recv()
        part = cols_chunk // 2

        def body(i, carry):
            cols = columns(q * cols_chunk + i * part, part)
            total = base_ref[pl.ds(my_inner * outer, outer), :, cols].astype(jnp.float32)
            for step in range(1, inner):
                total += side_ref[lax.rem(my_inner + step, inner), :, :, cols].astype(jnp.float32)
            part_ref[:, :, cols] = total.astype(jnp.bfloat16)
            return carry

        lax.fori_loop(0, cols_chunk // part, body, 0)
        own_copy(q).start()
        for step in range(1, outer):
            outer_copy(q, my_outer, step).start()

    def product(path, q, lhs):
        cols = pl.ds(q * cols_chunk, cols_chunk)
        rhs = t_ref[:, cols] if path else passed_ref[...]
        term = jnp.dot(lhs, rhs, preferred_element_type=jnp.float32)
        mine_ref[path, :, cols] = term[:half]
        theirs_ref[path, :, cols] = term[half:]
        pair_copy(path, q).start()

    def reduce_send(path, q):
        pair_copy(path, q).wait_recv()
        to_ref = base_ref if path else stage_ref
        part = cols_chunk // 2

        def body(i, carry):
            cols = columns(q * cols_chunk + i * part, part)
            total = (mine_ref[path, :, cols] + partner_ref[path, :, cols]).astype(jnp.bfloat16)
            for k in range(chips):
                to_ref[k, :, cols] = total[k * row_dev : (k + 1) * row_dev]
            return carry

        lax.fori_loop(0, cols_chunk // part, body, 0)
        if path == 0:
            down_copy(q).start()
        else:
            send_inner(q)

    def statistics_of(first_block, last_block):
        sub_rows = 32
        span = cols_chunk // 2

        def fold(value):
            parts = [value[:, i * LANES : (i + 1) * LANES] for i in range(span // LANES)]
            while len(parts) > 1:
                parts = [
                    parts[i] + parts[i + 1] if i + 1 < len(parts) else parts[i]
                    for i in range(0, len(parts), 2)
                ]
            return parts[0]

        def statistics(r, carry):
            at = pl.ds(pl.multiple_of(r * sub_rows, sub_rows), sub_rows)
            zero = jnp.zeros((sub_rows, LANES), jnp.float32)

            def first(i, sums):
                cols = columns(i * span, span)
                values = x_ref[at, cols].astype(jnp.float32)
                scaled = g_ref[at, cols].astype(jnp.float32) * gain_ref[:, cols]
                return (sums[0] + fold(values), sums[1] + fold(scaled))

            sums = lax.fori_loop(0, width // span, first, (zero, zero))
            mean = jnp.sum(sums[0], axis=-1, keepdims=True) / width
            mean_scaled = jnp.sum(sums[1], axis=-1, keepdims=True) / width

            def second(i, sums):
                cols = columns(i * span, span)
                centred = x_ref[at, cols].astype(jnp.float32) - mean
                scaled = g_ref[at, cols].astype(jnp.float32) * gain_ref[:, cols]
                return (sums[0] + fold(centred * centred), sums[1] + fold(scaled * centred))

            sums = lax.fori_loop(0, width // span, second, (zero, zero))
            var = jnp.sum(sums[0], axis=-1, keepdims=True) / width
            inv_std = 1.0 / jnp.sqrt(var + 1e-05)
            along = jnp.sum(sums[1], axis=-1, keepdims=True) / width * inv_std
            full = (sub_rows, LANES)
            stats_ref[0, at, :] = jnp.broadcast_to(mean, full)
            stats_ref[1, at, :] = jnp.broadcast_to(mean_scaled, full)
            stats_ref[2, at, :] = jnp.broadcast_to(along * inv_std, full)
            stats_ref[3, at, :] = jnp.broadcast_to(inv_std, full)
            return carry

        per_block = block_rows // sub_rows
        for b in range(first_block, last_block):
            x_loads[b].wait()
            g_loads[b].wait()
            lax.fori_loop(b * per_block, (b + 1) * per_block, statistics, 0)

    @pl.when(has_lower)
    def _():
        gain_load.wait()
        statistics_of(0, blocks)

    @pl.when(has_lower | is_last)
    def _():
        t_load.wait()

    @pl.when(has_lower)
    def _():
        hidden_copy.wait_recv()
        lhs = arranged(lower_ref)

        span = cols_chunk // 2
        pass_rows = 32

        def passed(q):
            def body(i, carry):
                at = pl.ds(pl.multiple_of(lax.rem(i, tokens // pass_rows) * pass_rows, pass_rows), pass_rows)
                cols = columns(q * cols_chunk + lax.div(i, tokens // pass_rows) * span, span)

                def wide(which):
                    return jnp.concatenate([stats_ref[which, at]] * (span // LANES), axis=1)

                centred = x_ref[at, cols].astype(jnp.float32) - wide(0)
                scaled = g_ref[at, cols].astype(jnp.float32) * gain_ref[:, cols]
                inner_term = (scaled - wide(1)) - centred * wide(2)
                passed_ref[at, pl.ds(pl.multiple_of(lax.div(i, tokens // pass_rows) * span, LANES), span)] = (
                    t_ref[at, cols].astype(jnp.float32) + inner_term * wide(3)
                ).astype(jnp.bfloat16)
                return carry

            lax.fori_loop(0, tokens // pass_rows * (cols_chunk // span), body, 0)

        for q in range(CHUNKS):
            passed(q)
            product(0, q, lhs)
            if q:
                reduce_send(0, q - 1)
        reduce_send(0, CHUNKS - 1)

    @pl.when(is_last)
    def _():
        hidden_load.wait()
        lhs = arranged(hidden_ref)
        for q in range(CHUNKS):
            product(1, q, lhs)
            if q:
                reduce_send(1, q - 1)
        reduce_send(1, CHUNKS - 1)

    def gather_copy(q, source, target):
        cols = pl.ds(q * cols_chunk, cols_chunk)
        return pltpu.make_async_remote_copy(
            src_ref=weights_ref.at[chip_dev(source), :, cols],
            dst_ref=weights_ref.at[chip_dev(source), :, cols],
            send_sem=ag_send.at[lax.div(source, inner), target, q],
            recv_sem=ag_recv.at[source, q],
            device_id=(sec, chip_dev(target)),
            device_id_type=MESH,
        )

    def forward_copy(q, source):
        cols = pl.ds(q * cols_chunk, cols_chunk)
        return pltpu.make_async_remote_copy(
            src_ref=weights_ref.at[chip_dev(source), :, cols],
            dst_ref=weights_ref.at[chip_dev(source), :, cols],
            send_sem=fw_send.at[source, q],
            recv_sem=fw_recv.at[source, q],
            device_id=(sec, partner),
            device_id_type=MESH,
        )

    for load in state_loads:
        load.wait()

    def finish_chunk(q):
        cols = pl.ds(q * cols_chunk, cols_chunk)
        for k in range(outer):
            pltpu.make_async_copy(
                recv_ref.at[k, :, cols], recv_ref.at[k, :, cols], outer_recv.at[k, q]
            ).wait()
        part = cols_chunk // 2

        def update(i, carry):
            at = columns(q * cols_chunk + i * part, part)
            grad = jnp.sum(recv_ref[:, :, at].astype(jnp.float32), axis=0)
            masters, moments, seconds = adam_update(
                grad, state_ref[0, :, at], state_ref[1, :, at], state_ref[2, :, at]
            )
            new_master_ref[:, at] = masters
            new_moment_ref[:, at] = moments
            new_second_ref[:, at] = seconds
            weights_ref[me, :, at] = masters.astype(jnp.bfloat16)
            return carry

        lax.fori_loop(0, cols_chunk // part, update, 0)
        for step in range(1, outer):
            gather_copy(q, chip, at_chip(step, 0)).start()
        for step in range(1, inner):
            gather_copy(q, chip, at_chip(0, step)).start()
        forward_copy(q, chip).start()

    for turn in range(CHUNKS + 2):

        if turn < CHUNKS:

            @pl.when(has_upper)
            def _():
                down_copy(turn).wait_recv()
                send_inner(turn)

        if 0 < turn <= CHUNKS:
            add_inner(turn - 1)
        if turn >= 2:
            finish_chunk(turn - 2)

    for q in range(CHUNKS):
        for outer_step in range(1, outer):
            source = at_chip(outer_step, 0)
            gather_copy(q, source, chip).wait_recv()
            for step in range(1, inner):
                gather_copy(q, source, at_chip(0, step)).start()
            forward_copy(q, source).start()
    for q in range(CHUNKS):
        for outer_step in range(outer):
            for step in range(1, inner):
                source = at_chip(outer_step, step)
                gather_copy(q, source, chip).wait_recv()
                forward_copy(q, source).start()

    for q in range(CHUNKS):
        for outer_step in range(outer):
            for step in range(inner):
                forward_copy(q, at_chip(outer_step, step)).wait()
            for step in range(1, inner):
                gather_copy(q, at_chip(outer_step, 0), at_chip(0, step)).wait_send()
            if outer_step:
                gather_copy(q, chip, at_chip(outer_step, 0)).wait_send()

    def finish(path):
        for q in range(CHUNKS):
            pair_copy(path, q).wait_send()
            if path == 0:
                down_copy(q).wait_send()

    for q in range(CHUNKS):
        for step in range(1, inner):
            inner_copy(q, my_inner, step).wait_send()
        for step in range(1, outer):
            outer_copy(q, my_outer, step).wait_send()

    @pl.when(has_lower)
    def _():
        finish(0)

    @pl.when(is_last)
    def _():
        finish(1)

    @pl.when(has_upper)
    def _():
        hidden_copy.wait_send()


def write_out(master, moment, second, gathered, new_master, new_moment, new_second, weights):
    new_master[...] = master[...]
    new_moment[...] = moment[...]
    new_second[...] = second[...]
    group, row_dev, _ = gathered.shape
    for owner in range(group):
        weights[owner * row_dev : (owner + 1) * row_dev] = gathered[owner]


def solution(mesh):
    sections = mesh.shape["section"]
    group = mesh.shape["dp"]
    chips = group // CORES
    inner = 1
    while inner * inner * 4 <= chips and chips % (inner * 2) == 0:
        inner *= 2

    def step(ln_input, ln_grad, top_grad, ln_gain, hidden, master, moment, second):
        tokens, width = ln_input.shape[1:]
        rows = hidden.shape[2]
        row_dev = master.shape[1]
        half = rows // CORES
        any_space = pl.BlockSpec(memory_space=pl.ANY)
        vmem = pl.BlockSpec(memory_space=pltpu.VMEM)
        state = jax.ShapeDtypeStruct((row_dev, width), jnp.float32)
        dma = pltpu.SemaphoreType.DMA
        outs = pl.pallas_call(
            functools.partial(kernel, sections, group, inner),
            out_shape=(
                state,
                state,
                state,
                jax.ShapeDtypeStruct((group, row_dev, width), jnp.bfloat16),
            ),
            in_specs=[any_space] * 8,
            out_specs=(vmem,) * 4,
            scratch_shapes=[
                pltpu.VMEM((tokens, width), jnp.bfloat16),
                pltpu.VMEM((tokens, width), jnp.bfloat16),
                pltpu.VMEM((tokens, width), jnp.bfloat16),
                pltpu.VMEM((tokens, width // CHUNKS), jnp.bfloat16),
                pltpu.VMEM((1, width), jnp.float32),
                pltpu.VMEM((rows, tokens), jnp.bfloat16),
                pltpu.VMEM((rows, tokens), jnp.bfloat16),
                pltpu.VMEM((3, row_dev, width), jnp.float32),
                pltpu.VMEM((4, tokens, LANES), jnp.float32),
                pltpu.VMEM((2, half, width), jnp.float32),
                pltpu.VMEM((2, half, width), jnp.float32),
                pltpu.VMEM((2, half, width), jnp.float32),
                pltpu.VMEM((chips, row_dev, width), jnp.bfloat16),
                pltpu.VMEM((chips, row_dev, width), jnp.bfloat16),
                pltpu.VMEM((inner, chips // inner, row_dev, width), jnp.bfloat16),
                pltpu.VMEM((chips // inner, row_dev, width), jnp.bfloat16),
                pltpu.VMEM((chips // inner, row_dev, width), jnp.bfloat16),
                dma((11,)),
                dma((3,)),
                dma,
                dma,
                dma((2, CHUNKS)),
                dma((2, CHUNKS)),
                dma((CHUNKS,)),
                dma((CHUNKS,)),
                dma((inner, CHUNKS)),
                dma((inner, CHUNKS)),
                dma((chips // inner, CHUNKS)),
                dma((chips // inner, CHUNKS)),
                dma((chips // inner, chips, CHUNKS)),
                dma((chips, CHUNKS)),
                dma((chips, CHUNKS)),
                dma((chips, CHUNKS)),
            ],
            compiler_params=pltpu.CompilerParams(
                collective_id=0, has_side_effects=True, vmem_limit_bytes=60 * 2**20
            ),
        )(
            ln_input[0],
            ln_grad[0],
            top_grad[0],
            ln_gain,
            hidden[0].T,
            master[0],
            moment[0],
            second[0],
        )
        slab = width // 2
        strip = pl.BlockSpec((row_dev, slab), lambda i: (0, i))
        masters, moments, seconds, weights = pl.pallas_call(
            write_out,
            grid=(width // slab,),
            out_shape=(state, state, state, jax.ShapeDtypeStruct((rows, width), jnp.bfloat16)),
            in_specs=[strip] * 3 + [pl.BlockSpec((group, row_dev, slab), lambda i: (0, 0, i))],
            out_specs=(strip,) * 3 + (pl.BlockSpec((rows, slab), lambda i: (0, i)),),
        )(*outs)
        return (masters[None], moments[None], seconds[None], weights[None])

    return jax.shard_map(
        step,
        mesh=mesh,
        in_specs=(
            P("section", "dp", None),
            P("section", "dp", None),
            P("section", "dp", None),
            P("section", None),
            P("section", "dp", None),
            P("section", "dp", None),
            P("section", "dp", None),
            P("section", "dp", None),
        ),
        out_specs=(
            P("section", "dp", None),
            P("section", "dp", None),
            P("section", "dp", None),
            P("section", None, None),
        ),
        check_vma=False,
    )
```
